32 devices in a mesh: groups: 2 (over y), dp: 4 (over z), layer: 4 (over x, core).
Axes of the slice: x: 2, y: 2, z: 4, core: 2. Of those that a mesh axis runs over, the one named last changes fastest.
Arguments:
- layer_inputs: float32 [4, 1024, 512], P('layer', ('groups', 'dp')), parts along dimension 1, may hold values from -6 to 6
- pre_acts: float32 [4, 1024, 512], P('layer', ('groups', 'dp')), parts along dimension 1, may hold values from -6 to 6
- layer_outputs: float32 [4, 1024, 512], P('layer', ('groups', 'dp')), parts along dimension 1, may hold values from -6 to 6
- multipliers: float32 [4, 1024, 512], P('layer', ('groups', 'dp')), parts along dimension 1, may hold values from -6 to 6
- weights: float32 [8, 512, 512], P(('groups', 'layer')), parts along dimension 0, may hold values from -0.25 to 0.25
- biases: float32 [8, 512], P(('groups', 'layer')), parts along dimension 0, may hold values from -3 to 3
- prev_outputs: float32 [1024, 512], P(('groups', 'dp')), parts along dimension 0, may hold values from -6 to 6
- prev_multipliers: float32 [1024, 512], P(('groups', 'dp')), parts along dimension 0, may hold values from -6 to 6
- next_inputs: float32 [1024, 512], P(('groups', 'dp')), parts along dimension 0, may hold values from -6 to 6
- row_order: int32 [8, 128], P(('groups', 'dp')), parts along dimension 0, may hold values from 0 to 127, each once within a row
Outputs:
- new_inputs: float32 [4, 1024, 512], P('layer', ('groups', 'dp')), parts along dimension 1
- new_preacts: float32 [4, 1024, 512], P('layer', ('groups', 'dp')), parts along dimension 1
- new_outputs: float32 [4, 1024, 512], P('layer', ('groups', 'dp')), parts along dimension 1
- new_multipliers: float32 [4, 1024, 512], P('layer', ('groups', 'dp')), parts along dimension 1
- new_weights: float32 [8, 512, 512], P(('groups', 'layer')), parts along dimension 0
- new_biases: float32 [8, 512], P(('groups', 'layer')), parts along dimension 0
The draws below stay inside these ranges and needn't reach their ends.
There are 2 independent parts, one for each index of `groups`. The reference program is written for one: setup_inputs(seed, part) draws one part's arguments, and reference() takes and returns one part's arrays. A program takes and returns all parts, laid end to end along the dimension named above; each array names one. Nothing has to cross between parts.
Inputs may be any that keep to these rules, and one draw needn't show every extreme that they name: Each row of row_order holds every number of 0 to 127 once.
All inputs are finite; a program needn't handle non-finite values.
Results may differ from the reference program's by a relative error of at most 0.0001.
Values sent between devices are 32-bit elements; how exact they have to be, the bound alone decides.
No kernel may reach another device: no remote copies, remote signals or barrier semaphores. Data moves between devices by JAX's collectives and lax.ppermute only.
A program may use at most 64 MiB of HBM per device.

```python
import jax
import jax.numpy as jnp
from jax import lax

D = 512
ROWS = 128
INNER = 3
PASSES = 1
NODES = 512
LAYERS = 4
N_DP = 4


def block_scale(stream_key, extent, cuts, least, largest):
    loudness = 1.0
    for position, shards_of in cuts:
        draws = jax.random.uniform(jax.random.fold_in(jax.random.fold_in(stream_key, 6), position), (shards_of,), jnp.float32, least / len(cuts), largest / len(cuts))
        loudness = loudness * jnp.repeat(jnp.exp(draws), extent[position] // shards_of).reshape((-1,) + (1,) * (len(extent) - 1 - position))
    return loudness


def gaussian(stream_key, shape, width, most, cuts=(), held_as=jnp.bfloat16):
    values = width * jax.random.normal(stream_key, shape, jnp.float32)
    if cuts:
        values = values * block_scale(stream_key, shape, cuts, -0.22, 0.18)
    return jnp.clip(values, -most, most).astype(held_as)


def setup_inputs(seed: int = 0, part: int = 0) -> dict:
    key_of = jax.random.split(jax.random.key(seed), 11)
    part_splits = jax.random.split(jax.random.fold_in(key_of[10], part), 11)
    return {
        "layer_inputs": gaussian(part_splits[0], (LAYERS, NODES, D), 1.0, 6.0, ((0, 4), (1, 4)), jnp.float32),
        "pre_acts": gaussian(part_splits[1], (LAYERS, NODES, D), 1.0, 6.0, ((0, 4), (1, 4)), jnp.float32),
        "layer_outputs": gaussian(part_splits[2], (LAYERS, NODES, D), 1.0, 6.0, ((0, 4), (1, 4)), jnp.float32),
        "multipliers": gaussian(part_splits[3], (LAYERS, NODES, D), 1.0, 6.0, ((0, 4), (1, 4)), jnp.float32),
        "weights": gaussian(part_splits[4], (LAYERS, D, D), D ** -0.5, 0.25, ((0, 4),), jnp.float32),
        "biases": gaussian(part_splits[5], (LAYERS, D), 0.5, 3.0, ((0, 4),), jnp.float32),
        "prev_outputs": gaussian(part_splits[6], (NODES, D), 1.0, 6.0, ((0, 4),), jnp.float32),
        "prev_multipliers": gaussian(part_splits[7], (NODES, D), 1.0, 6.0, ((0, 4),), jnp.float32),
        "next_inputs": gaussian(part_splits[8], (NODES, D), 1.0, 6.0, ((0, 4),), jnp.float32),
        "row_order": jax.vmap(lambda own: jax.random.permutation(own, ROWS))(jax.random.split(part_splits[9], N_DP)).reshape((N_DP, ROWS)).astype(jnp.int32),
    }


penalty_nu = 1.0
penalty_rho = 1.0
step_input = 0.2
step_weight = 0.3
step_preact = 0.5


def matmul(form, left, right):
    return jnp.einsum(form, left, right, precision=lax.Precision.HIGHEST)


def reference(layer_inputs, pre_acts, layer_outputs, multipliers, weights, biases, prev_outputs, prev_multipliers, next_inputs, row_order):
    blocks = row_order.shape[0]
    base = (jnp.arange(blocks, dtype=jnp.int32) * ROWS)[:, None]
    gathered = (row_order.astype(jnp.int32) + base).reshape(-1)
    edge_outputs = jnp.take(prev_outputs, gathered, axis=0)
    edge_duals = jnp.take(prev_multipliers, gathered, axis=0)
    edge_inputs = jnp.take(next_inputs, gathered, axis=0)
    row_count = layer_inputs.shape[1]
    inputs, preact, outputs, duals = layer_inputs, pre_acts, layer_outputs, multipliers
    weight, offset = weights, biases
    for outer_pass in range(PASSES):
        before_out = jnp.concatenate([edge_outputs[None], outputs[:-1]], axis=0)
        before_dual = jnp.concatenate([edge_duals[None], duals[:-1]], axis=0)
        residual = matmul("lmd,lde->lme", inputs, weight) + offset[:, None, :] - preact
        back = matmul("lme,lde->lmd", residual, weight)
        inputs = inputs - step_input * (penalty_nu * back + before_dual + penalty_rho * (inputs - before_out))
        for inner_step in range(INNER):
            residual = matmul("lmd,lde->lme", inputs, weight) + offset[:, None, :] - preact
            grad_weight = matmul("lmd,lme->lde", inputs, residual)
            grad_offset = jnp.sum(residual, axis=1)
            weight = weight - (step_weight / row_count) * grad_weight
            offset = offset - (step_weight / row_count) * grad_offset
        target = matmul("lmd,lde->lme", inputs, weight) + offset[:, None, :]
        preact = preact - step_preact * ((preact - target) + (jax.nn.softplus(preact) - outputs) * jax.nn.sigmoid(preact))
        after_in = jnp.concatenate([inputs[1:], edge_inputs[None]], axis=0)
        outputs = (penalty_nu * jax.nn.softplus(preact) + duals + penalty_rho * after_in) / (penalty_nu + penalty_rho)
        duals = duals + penalty_rho * (after_in - outputs)
    return inputs, preact, outputs, duals, weight, offset
```

```python
import jax
import jax.numpy as jnp
from jax import lax
from jax.sharding import PartitionSpec as P

INNER = 3


penalty_nu = 1.0
penalty_rho = 1.0
step_input = 0.2
step_weight = 0.3
step_preact = 0.5


def from_behind(x, axis, by):
    count = lax.axis_size(axis)
    pairs = [(i, i + by) for i in range(count) if 0 <= i + by < count]
    return lax.ppermute(x, axis, pairs)


def matmul(left, right):
    return jnp.dot(left, right, precision=lax.Precision.HIGHEST)


def line_plan(count):
    outbox = {(i, side): [i] for i in range(count) for side in (-1, 1)}
    rounds = []
    while any(outbox[i, side] for i in range(count) for side in (-1, 1) if 0 <= i + side < count):
        for parity in (0, 1):
            sends = []
            for i in range(count):
                side = 1 if i % 2 == parity else -1
                if 0 <= i + side < count and outbox[i, side]:
                    sends.append((i, i + side, outbox[i, side].pop(0)))
            for source, target, block in sends:
                outbox[target, target - source].append(block)
            if sends:
                rounds.append(sends)
    return rounds


def gather_line(own, axis):
    count = lax.axis_size(axis)
    me = lax.axis_index(axis)
    held = {(i, i): own for i in range(count)}
    slots = [[] for _ in range(count - 1)]
    got = [0] * count
    for sends in line_plan(count):
        by_value = {}
        for source, target, block in sends:
            value = held[source, block]
            by_value.setdefault(id(value), (value, []))[1].append(source)
        (payload, _), *others = by_value.values()
        for value, sources in others:
            mine = jnp.any(jnp.asarray(sources) == me)
            payload = jnp.where(mine, value, payload)
        arrived = lax.ppermute(payload, axis, [(s, t) for s, t, _ in sends])
        per_slot = {}
        for source, target, block in sends:
            held[target, block] = arrived
            per_slot.setdefault(got[target], []).append(target)
            got[target] += 1
        for slot, members in per_slot.items():
            slots[slot].append((arrived, members))
    merged = []
    for parts in slots:
        value = parts[0][0]
        for other, members in parts[1:]:
            value = jnp.where(jnp.any(jnp.asarray(members) == me), other, value)
        merged.append(value)
    return merged


def summed_steps(inputs, preact, weight, offset, scale):
    row_count = inputs.shape[0] * lax.axis_size("dp")
    gram_matrix, cross_term, column_sums, preact_sums = lax.psum(
        (
            matmul(inputs.T, inputs),
            matmul(inputs.T, preact),
            jnp.sum(inputs, axis=0),
            jnp.sum(preact, axis=0),
        ),
        "dp",
    )
    for inner_step in range(INNER):
        grad_weight = (
            matmul(gram_matrix, weight) + column_sums[:, None] * offset[None, :] - cross_term
        )
        grad_offset = matmul(column_sums[None, :], weight)[0] + row_count * offset - preact_sums
        weight = weight - scale * grad_weight
        offset = offset - scale * grad_offset
    return weight, offset


def gathered_steps(inputs, preact_rows, weight, offset, scale):
    rows = jnp.concatenate([inputs] + gather_line(inputs, "dp"), axis=0)
    late = inputs.shape[0] * (lax.axis_size("dp") - 1)
    kernel = scale * (matmul(rows, rows.T) + 1.0)
    eye = jnp.eye(rows.shape[0], dtype=rows.dtype)
    total = eye
    for inner_step in range(1, INNER):
        total = eye + total - (matmul(kernel, total) if inner_step > 1 else kernel)
    pull = scale * matmul(rows.T, total)
    pull_offset = scale * jnp.sum(total, axis=0)
    early_rows = jnp.concatenate(
        preact_rows[:-1] + [jnp.zeros_like(preact_rows[-1])], axis=0
    )
    residual = matmul(rows, weight) + offset[None, :] - early_rows
    weight = weight - matmul(pull, residual)
    offset = offset - matmul(pull_offset[None, :], residual)[0]
    weight = weight + matmul(pull[:, late:], preact_rows[-1])
    offset = offset + matmul(pull_offset[None, late:], preact_rows[-1])[0]
    return weight, offset


def body(
    layer_inputs,
    pre_acts,
    layer_outputs,
    multipliers,
    weights,
    biases,
    prev_outputs,
    prev_multipliers,
    next_inputs,
    row_order,
):
    row_perm = row_order[0]
    first_layer = lax.axis_index("layer") == 0
    last_layer = lax.axis_index("layer") == lax.axis_size("layer") - 1
    inputs, preact, outputs, duals = (
        layer_inputs[0],
        pre_acts[0],
        layer_outputs[0],
        multipliers[0],
    )
    weight, offset = (weights[0], biases[0])
    row_count = inputs.shape[0] * lax.axis_size("dp")
    scale = step_weight / row_count
    gathers = row_count <= 2 * inputs.shape[1]
    before = from_behind(duals - penalty_rho * outputs, "layer", 1)
    if gathers:
        preact_rows = [preact] + gather_line(preact, "dp")
    edge_before = jnp.take(prev_multipliers - penalty_rho * prev_outputs, row_perm, axis=0)
    before = jnp.where(first_layer, edge_before, before)
    residual = matmul(inputs, weight) + offset[None, :] - preact
    inputs = inputs - step_input * (
        penalty_nu * matmul(residual, weight.T) + penalty_rho * inputs + before
    )
    after_in = from_behind(inputs, "layer", -1)
    if gathers:
        weight, offset = gathered_steps(inputs, preact_rows, weight, offset, scale)
    else:
        weight, offset = summed_steps(inputs, preact, weight, offset, scale)
    target = matmul(inputs, weight) + offset[None, :]
    preact = preact - step_preact * (
        preact - target + (jax.nn.softplus(preact) - outputs) * jax.nn.sigmoid(preact)
    )
    edge_inputs = jnp.take(next_inputs, row_perm, axis=0)
    after_in = jnp.where(last_layer, edge_inputs, after_in)
    outputs = (penalty_nu * jax.nn.softplus(preact) + duals + penalty_rho * after_in) / (
        penalty_nu + penalty_rho
    )
    duals = duals + penalty_rho * (after_in - outputs)
    return (inputs[None], preact[None], outputs[None], duals[None], weight[None], offset[None])


def solution(mesh):
    return jax.shard_map(
        body,
        mesh=mesh,
        in_specs=(
            P("layer", ("groups", "dp"), None),
            P("layer", ("groups", "dp"), None),
            P("layer", ("groups", "dp"), None),
            P("layer", ("groups", "dp"), None),
            P(("groups", "layer"), None, None),
            P(("groups", "layer"), None),
            P(("groups", "dp"), None),
            P(("groups", "dp"), None),
            P(("groups", "dp"), None),
            P(("groups", "dp"), None),
        ),
        out_specs=(
            P("layer", ("groups", "dp"), None),
            P("layer", ("groups", "dp"), None),
            P("layer", ("groups", "dp"), None),
            P("layer", ("groups", "dp"), None),
            P(("groups", "layer"), None, None),
            P(("groups", "layer"), None),
        ),
        check_vma=False,
    )
```

```python
import jax
import jax.numpy as jnp
from jax import lax
from jax.experimental import pallas as pl
from jax.experimental.pallas import tpu as pltpu
from jax.sharding import PartitionSpec as P


INNER = 3


penalty_nu = 1.0
penalty_rho = 1.0
step_input = 0.2
step_weight = 0.3
step_preact = 0.5


def from_behind(x, axis, by):
    count = lax.axis_size(axis)
    pairs = [(i, i + by) for i in range(count) if 0 <= i + by < count]
    return lax.ppermute(x, axis, pairs)


def matmul(left, right):
    return jnp.dot(left, right, precision=lax.Precision.HIGHEST)


def line_plan(count):
    outbox = {(i, side): [i] for i in range(count) for side in (-1, 1)}
    rounds = []
    while any(outbox[i, side] for i in range(count) for side in (-1, 1) if 0 <= i + side < count):
        for parity in (0, 1):
            sends = []
            for i in range(count):
                side = 1 if i % 2 == parity else -1
                if 0 <= i + side < count and outbox[i, side]:
                    sends.append((i, i + side, outbox[i, side].pop(0)))
            for source, target, block in sends:
                outbox[target, target - source].append(block)
            if sends:
                rounds.append(sends)
    return rounds


def gather_line(own, axis):
    count = lax.axis_size(axis)
    me = lax.axis_index(axis)
    held = {(i, i): own for i in range(count)}
    slots = [[] for _ in range(count - 1)]
    got = [0] * count
    for sends in line_plan(count):
        by_value = {}
        for source, target, block in sends:
            value = held[source, block]
            by_value.setdefault(id(value), (value, []))[1].append(source)
        (payload, _), *others = by_value.values()
        for value, sources in others:
            mine = jnp.any(jnp.asarray(sources) == me)
            payload = jnp.where(mine, value, payload)
        arrived = lax.ppermute(payload, axis, [(s, t) for s, t, _ in sends])
        filled = []
        for source, target, block in sends:
            held[target, block] = arrived
            if got[target] not in filled:
                filled.append(got[target])
            got[target] += 1
        for slot in filled:
            slots[slot].append(arrived)
    return slots


def summed_steps(inputs, preact, weight, offset, scale):
    row_count = inputs.shape[0] * lax.axis_size("dp")
    gram_matrix, cross_term, column_sums, preact_sums = lax.psum(
        (
            matmul(inputs.T, inputs),
            matmul(inputs.T, preact),
            jnp.sum(inputs, axis=0),
            jnp.sum(preact, axis=0),
        ),
        "dp",
    )
    for _ in range(INNER):
        grad_weight = (
            matmul(gram_matrix, weight) + column_sums[:, None] * offset[None, :] - cross_term
        )
        grad_offset = matmul(column_sums[None, :], weight)[0] + row_count * offset - preact_sums
        weight = weight - scale * grad_weight
        offset = offset - scale * grad_offset
    return weight, offset


VMEM = pl.BlockSpec(memory_space=pltpu.VMEM)
HBM = pl.BlockSpec(memory_space=pltpu.HBM)
NN = (((1,), (0,)), ((), ()))
NT = (((1,), (1,)), ((), ()))


def f32(*shape):
    return jax.ShapeDtypeStruct(shape, jnp.float32)


def bf16(*shape):
    return jax.ShapeDtypeStruct(shape, jnp.bfloat16)


def run(kernel, args, outs, flops, out_specs=None, scratch=()):
    nbytes = sum(x.size * x.dtype.itemsize for x in (*args, *outs))
    return pl.pallas_call(
        kernel,
        out_shape=outs,
        in_specs=[VMEM] * len(args),
        out_specs=[VMEM] * len(outs) if out_specs is None else out_specs,
        scratch_shapes=scratch,
        cost_estimate=pl.CostEstimate(flops=flops, bytes_accessed=nbytes, transcendentals=0),
        compiler_params=pltpu.CompilerParams(vmem_limit_bytes=24 * 2**20),
    )(*args)


def split(x):
    high = x.astype(jnp.bfloat16)
    return high, (x - high.astype(jnp.float32)).astype(jnp.bfloat16)


def dot3(left, right, dims=NN):
    one = lambda a, b: lax.dot_general(a, b, dims, preferred_element_type=jnp.float32)
    return one(left[0], right[0]) + (one(left[0], right[1]) + one(left[1], right[0]))


def pick_rows(rows, order):
    count = rows.shape[0]
    hot = (lax.broadcasted_iota(jnp.int32, (count, count), 0) == order).astype(jnp.float32)
    hot = hot.T.astype(jnp.bfloat16)
    high, low = split(rows)
    rest = (rows - high.astype(jnp.float32) - low.astype(jnp.float32)).astype(jnp.bfloat16)
    one = lambda b: lax.dot_general(hot, b, NN, preferred_element_type=jnp.float32)
    return one(high) + (one(low) + one(rest))


def softplus(v):
    return jnp.maximum(v, 0.0) + jnp.log1p(jnp.exp(-jnp.abs(v)))


def minus_kernel(u, q, out):
    out[...] = u[0] - penalty_rho * q[0]


def input_kernel(p, z, w, b, qb, ub, order, out):
    weight = split(w[0])
    residual = dot3(split(p[0]), weight) + b[...] - z[0]
    step = penalty_nu * dot3(split(residual), weight, NT) + penalty_rho * p[0]
    out[...] = p[0] - step_input * step

    @pl.when(lax.axis_index("layer") == 0)
    def _():
        out[...] -= step_input * pick_rows(ub[...] - penalty_rho * qb[...], order[...])


def total_of(refs):
    value = refs[0][...]
    for ref in refs[1:]:
        value = value + ref[...]
    return value


def gathered_pass(inputs, preact, outputs, duals, weight, offset, after_in, next_inputs, row_order, p_slots, z_slots, scale):
    rows, width = inputs.shape
    early_count = rows * len(p_slots)
    count = early_count + rows
    p_early = [[inputs]] + p_slots[:-1]
    z_early = [[preact[0]]] + z_slots[:-1]
    p_late, z_late = p_slots[-1], z_slots[-1]
    sizes = [len(parts) for parts in p_early]
    unit = 2 * rows * width * width * 3

    def group(refs, counts):
        out = []
        for n in counts:
            out.append(refs[:n])
            refs = refs[n:]
        return out

    def early_kernel(*refs):
        ins = refs[: 2 * sum(sizes)]
        w, b, z, q, u, pn, pb, order = refs[2 * sum(sizes) : 2 * sum(sizes) + 8]
        residual, kernel, z_part, q_part = refs[2 * sum(sizes) + 8 :]
        p_refs, z_refs = group(ins[: sum(sizes)], sizes), group(ins[sum(sizes) :], sizes)
        wide = split(w[0])
        blocks = [split(total_of(r)) for r in p_refs]
        for i, block in enumerate(blocks):
            at = slice(i * rows, (i + 1) * rows)
            residual[at] = dot3(block, wide) + b[...] - total_of(z_refs[i])
            for j in range(i + 1):
                to = slice(j * rows, (j + 1) * rows)
                piece = scale * (dot3(block, blocks[j], NT) + 1.0)
                kernel[at, to] = piece
                if j < i:
                    kernel[to, at] = piece.T
        value = z[0]
        z_part[...] = (1 - step_preact) * value - step_preact * (
            (softplus(value) - q[0]) * jax.nn.sigmoid(value)
        )
        q_part[...] = u[0] + penalty_rho * pn[...]

        @pl.when(lax.axis_index("layer") == lax.axis_size("layer") - 1)
        def _():
            q_part[...] += penalty_rho * pick_rows(pb[...], order[...])

    args = [x for parts in p_early for x in parts] + [x for parts in z_early for x in parts]
    args += [weight, offset, preact, outputs, duals, after_in, next_inputs, row_order]
    residual, kernel, z_part, q_part = run(
        early_kernel,
        args,
        [f32(early_count, width), f32(early_count, early_count), f32(rows, width), f32(rows, width)],
        unit * (2 * len(sizes)),
    )

    def solve_kernel(*refs):
        ins = refs[: sum(sizes) + len(p_late)]
        residual, kernel, w, b = refs[len(ins) : len(ins) + 4]
        w_part, b_part, pull_high, pull_low, weigh, a_part, a_pull = refs[len(ins) + 4 : len(ins) + 11]
        j_ref, turned = refs[len(ins) + 11 :]
        wide = split(w[0])
        every = [total_of(r) for r in group(ins, sizes + [len(p_late)])]
        late = split(every[-1])
        j_ref[:early_count, :early_count] = kernel[...]
        for i, block in enumerate(every):
            at = slice(i * rows, (i + 1) * rows)
            turned[:, at] = block.T
            piece = scale * (dot3(split(block), late, NT) + 1.0)
            j_ref[at, early_count:] = piece
            if i * rows < early_count:
                j_ref[early_count:, at] = piece.T
        j = j_ref[...]
        both = split(j)
        eye = (
            lax.broadcasted_iota(jnp.int32, (count, count), 0)
            == lax.broadcasted_iota(jnp.int32, (count, count), 1)
        ).astype(jnp.float32)
        total = eye
        for inner_step in range(1, INNER):
            total = eye + total - (dot3(both, split(total)) if inner_step > 1 else j)
        pull = scale * dot3(split(turned[...]), split(total))
        sums = scale * jnp.sum(total, axis=1, keepdims=True)
        start = jnp.concatenate([residual[...], dot3(late, wide) + b[...]], axis=0)
        new = w[0] - dot3(split(pull), split(start))
        w_part[...] = new
        new_b = b[...] - jnp.sum(sums * start, axis=0, keepdims=True)
        b_part[...] = new_b
        pull_high[...], pull_low[...] = split(pull[:, early_count:])
        weigh[...] = jnp.broadcast_to(sums[early_count:], weigh.shape)
        own = split(every[0])
        a_part[...] = dot3(own, split(new)) + new_b
        a_pull[...] = dot3(own, (pull_high[...], pull_low[...]))

    args = [x for parts in p_early + [p_late] for x in parts] + [residual, kernel, weight, offset]
    solved = run(
        solve_kernel,
        args,
        [
            f32(width, width),
            f32(1, width),
            bf16(width, rows),
            bf16(width, rows),
            f32(rows, 128),
            f32(rows, width),
            f32(rows, rows),
        ],
        unit * (3 * len(p_slots) + 4),
        scratch=[pltpu.VMEM((count, count), jnp.float32), pltpu.VMEM((width, count), jnp.float32)],
    )

    def last_kernel(*refs):
        late_refs = refs[: len(z_late)]
        w_part, b_part, pull_high, pull_low, weigh, a_part, a_pull, z_part, q_part = refs[
            len(z_late) : len(z_late) + 9
        ]
        z_out, q_out, u_out, w_out, b_out = refs[len(z_late) + 9 : len(z_late) + 14]
        z_own, q_own, u_own, w_own, b_own, sems = refs[len(z_late) + 14 :]
        value = total_of(late_refs)
        late = split(value)
        new_w = w_part[...] + dot3((pull_high[...], pull_low[...]), late)
        w_own[0] = new_w
        copies = [pltpu.make_async_copy(w_own, w_out, sems.at[0])]
        copies[-1].start()
        shift = jnp.sum(weigh[:, :1] * value, axis=0, keepdims=True)
        b_own[...] = b_part[...] + shift
        copies.append(pltpu.make_async_copy(b_own, b_out, sems.at[1]))
        copies[-1].start()
        target = a_part[...] + shift + dot3(split(a_pull[...]), late)
        new_z = z_part[...] + step_preact * target
        z_own[0] = new_z
        copies.append(pltpu.make_async_copy(z_own, z_out, sems.at[2]))
        copies[-1].start()
        both = q_part[...]
        new_q = (penalty_nu * softplus(new_z) + both) / (penalty_nu + penalty_rho)
        q_own[0] = new_q
        copies.append(pltpu.make_async_copy(q_own, q_out, sems.at[3]))
        copies[-1].start()
        u_own[0] = both - penalty_rho * new_q
        copies.append(pltpu.make_async_copy(u_own, u_out, sems.at[4]))
        copies[-1].start()
        for copy in copies:
            copy.wait()

    one = f32(1, rows, width)
    outs = [one, one, one, f32(1, width, width), f32(1, width)]
    return run(
        last_kernel,
        list(z_late) + list(solved) + [z_part, q_part],
        outs,
        unit * 2,
        out_specs=[HBM] * len(outs),
        scratch=[pltpu.VMEM(o.shape, jnp.float32) for o in outs] + [pltpu.SemaphoreType.DMA((5,))],
    )


def gathered_body(
    layer_inputs, pre_acts, layer_outputs, multipliers, weights, biases,
    prev_outputs, prev_multipliers, next_inputs, row_order,
):
    rows, width = layer_inputs.shape[1:]
    scale = step_weight / (rows * lax.axis_size("dp"))
    unit = 2 * rows * width * width * 3
    z_slots = gather_line(pre_acts[0], "dp")
    (before,) = run(minus_kernel, (multipliers, layer_outputs), [f32(rows, width)], unit // 10)
    before = from_behind(before, "layer", 1)
    (inputs,) = run(
        input_kernel,
        (layer_inputs, pre_acts, weights, biases, prev_outputs, prev_multipliers, row_order),
        [f32(rows, width)],
        unit * 2,
    )
    inputs = inputs - step_input * before
    p_slots = gather_line(inputs, "dp")
    after_in = from_behind(inputs, "layer", -1)
    z, q, u, w, b = gathered_pass(
        inputs, pre_acts, layer_outputs, multipliers, weights, biases,
        after_in, next_inputs, row_order, p_slots, z_slots, scale,
    )
    return (inputs[None], z, q, u, w, b)


def summed_body(
    layer_inputs,
    pre_acts,
    layer_outputs,
    multipliers,
    weights,
    biases,
    prev_outputs,
    prev_multipliers,
    next_inputs,
    row_order,
):
    row_perm = row_order[0]
    first_layer = lax.axis_index("layer") == 0
    last_layer = lax.axis_index("layer") == lax.axis_size("layer") - 1
    inputs, preact, outputs, duals = (
        layer_inputs[0],
        pre_acts[0],
        layer_outputs[0],
        multipliers[0],
    )
    weight, offset = (weights[0], biases[0])
    row_count = inputs.shape[0] * lax.axis_size("dp")
    scale = step_weight / row_count
    before = from_behind(duals - penalty_rho * outputs, "layer", 1)
    edge_before = jnp.take(prev_multipliers - penalty_rho * prev_outputs, row_perm, axis=0)
    before = jnp.where(first_layer, edge_before, before)
    residual = matmul(inputs, weight) + offset[None, :] - preact
    inputs = inputs - step_input * (
        penalty_nu * matmul(residual, weight.T) + penalty_rho * inputs + before
    )
    after_in = from_behind(inputs, "layer", -1)
    weight, offset = summed_steps(inputs, preact, weight, offset, scale)
    target = matmul(inputs, weight) + offset[None, :]
    preact = preact - step_preact * (
        preact - target + (jax.nn.softplus(preact) - outputs) * jax.nn.sigmoid(preact)
    )
    edge_inputs = jnp.take(next_inputs, row_perm, axis=0)
    after_in = jnp.where(last_layer, edge_inputs, after_in)
    outputs = (penalty_nu * jax.nn.softplus(preact) + duals + penalty_rho * after_in) / (
        penalty_nu + penalty_rho
    )
    duals = duals + penalty_rho * (after_in - outputs)
    return (inputs[None], preact[None], outputs[None], duals[None], weight[None], offset[None])


def body(*args):
    inputs = args[0]
    count = lax.axis_size("dp")
    gathers = 1 < count and inputs.shape[1] * count <= 2 * inputs.shape[2]
    return (gathered_body if gathers else summed_body)(*args)


def solution(mesh):
    return jax.shard_map(
        body,
        mesh=mesh,
        in_specs=(
            P("layer", ("groups", "dp"), None),
            P("layer", ("groups", "dp"), None),
            P("layer", ("groups", "dp"), None),
            P("layer", ("groups", "dp"), None),
            P(("groups", "layer"), None, None),
            P(("groups", "layer"), None),
            P(("groups", "dp"), None),
            P(("groups", "dp"), None),
            P(("groups", "dp"), None),
            P(("groups", "dp"), None),
        ),
        out_specs=(
            P("layer", ("groups", "dp"), None),
            P("layer", ("groups", "dp"), None),
            P("layer", ("groups", "dp"), None),
            P("layer", ("groups", "dp"), None),
            P(("groups", "layer"), None, None),
            P(("groups", "layer"), None),
        ),
        check_vma=False,
    )
```

```python
import jax
import jax.numpy as jnp
from jax import lax
from jax.experimental import pallas as pl
from jax.experimental.pallas import tpu as pltpu
from jax.sharding import PartitionSpec as P


INNER = 3


penalty_nu = 1.0
penalty_rho = 1.0
step_input = 0.2
step_weight = 0.3
step_preact = 0.5


def from_behind(x, axis, by):
    count = lax.axis_size(axis)
    pairs = [(i, i + by) for i in range(count) if 0 <= i + by < count]
    return lax.ppermute(x, axis, pairs)


def matmul(left, right):
    return jnp.dot(left, right, precision=lax.Precision.HIGHEST)


def line_plan(count):
    outbox = {(i, side): [i] for i in range(count) for side in (-1, 1)}
    rounds = []
    while any(outbox[i, side] for i in range(count) for side in (-1, 1) if 0 <= i + side < count):
        for parity in (0, 1):
            sends = []
            for i in range(count):
                side = 1 if i % 2 == parity else -1
                if 0 <= i + side < count and outbox[i, side]:
                    sends.append((i, i + side, outbox[i, side].pop(0)))
            for source, target, block in sends:
                outbox[target, target - source].append(block)
            if sends:
                rounds.append(sends)
    return rounds


def whole_swap(swaps):
    layers = lax.axis_size("layer")
    pairs = []
    for i in range(lax.axis_size("dp")):
        for l in range(layers):
            partner = l ^ 1 if layers % 2 == 0 else l
            there = (swaps[i], l) if i in swaps else (i, partner)
            pairs.append((i * layers + l, there[0] * layers + there[1]))
    return pairs


def around(x, by):
    count = lax.axis_size("layer")
    return lax.ppermute(x, "layer", [(i, (i + by) % count) for i in range(count)])


def gather_line(own, axis):
    count = lax.axis_size(axis)
    me = lax.axis_index(axis)
    held = {(i, i): own for i in range(count)}
    slots = [[] for _ in range(count - 1)]
    got = [0] * count
    for sends in line_plan(count):
        by_value = {}
        for source, target, block in sends:
            value = held[source, block]
            by_value.setdefault(id(value), (value, []))[1].append(source)
        (payload, _), *others = by_value.values()
        for value, sources in others:
            mine = jnp.any(jnp.asarray(sources) == me)
            payload = jnp.where(mine, value, payload)
        swaps = dict((s, t) for s, t, _ in sends) | dict((t, s) for s, t, _ in sends)
        arrived = lax.ppermute(payload, ("dp", "layer"), whole_swap(swaps))
        filled = {}
        for source, target, block in sends:
            held[target, block] = arrived
            filled.setdefault(got[target], []).append(target)
            got[target] += 1
        for slot, members in filled.items():
            slots[slot].append((arrived, members))
    return slots


def summed_steps(inputs, preact, weight, offset, scale):
    row_count = inputs.shape[0] * lax.axis_size("dp")
    gram_matrix, cross_term, column_sums, preact_sums = lax.psum(
        (
            matmul(inputs.T, inputs),
            matmul(inputs.T, preact),
            jnp.sum(inputs, axis=0),
            jnp.sum(preact, axis=0),
        ),
        "dp",
    )
    for _ in range(INNER):
        grad_weight = (
            matmul(gram_matrix, weight) + column_sums[:, None] * offset[None, :] - cross_term
        )
        grad_offset = matmul(column_sums[None, :], weight)[0] + row_count * offset - preact_sums
        weight = weight - scale * grad_weight
        offset = offset - scale * grad_offset
    return weight, offset


VMEM = pl.BlockSpec(memory_space=pltpu.VMEM)
HBM = pl.BlockSpec(memory_space=pltpu.HBM)
NN = (((1,), (0,)), ((), ()))
NT = (((1,), (1,)), ((), ()))


def f32(*shape):
    return jax.ShapeDtypeStruct(shape, jnp.float32)


def bf16(*shape):
    return jax.ShapeDtypeStruct(shape, jnp.bfloat16)


def run(kernel, args, outs, flops, in_specs=None, out_specs=None, scratch=(), limit=24 * 2**20):
    nbytes = sum(x.size * x.dtype.itemsize for x in (*args, *outs))
    return pl.pallas_call(
        kernel,
        out_shape=outs,
        in_specs=[VMEM] * len(args) if in_specs is None else in_specs,
        out_specs=[VMEM] * len(outs) if out_specs is None else out_specs,
        scratch_shapes=scratch,
        cost_estimate=pl.CostEstimate(flops=flops, bytes_accessed=nbytes, transcendentals=0),
        compiler_params=pltpu.CompilerParams(vmem_limit_bytes=limit),
    )(*args)


def split(x):
    high = x.astype(jnp.bfloat16)
    return high, (x - high.astype(jnp.float32)).astype(jnp.bfloat16)


def dot3(left, right, dims=NN):
    one = lambda a, b: lax.dot_general(a, b, dims, preferred_element_type=jnp.float32)
    return one(left[0], right[0]) + (one(left[0], right[1]) + one(left[1], right[0]))


def pick_rows(rows, order):
    count = rows.shape[0]
    hot = (lax.broadcasted_iota(jnp.int32, (count, count), 0) == order).astype(jnp.float32)
    hot = hot.T.astype(jnp.bfloat16)
    high, low = split(rows)
    rest = (rows - high.astype(jnp.float32) - low.astype(jnp.float32)).astype(jnp.bfloat16)
    one = lambda b: lax.dot_general(hot, b, NN, preferred_element_type=jnp.float32)
    return one(high) + (one(low) + one(rest))


def softplus(v):
    return jnp.maximum(v, 0.0) + jnp.log1p(jnp.exp(-jnp.abs(v)))


def fetch(sources, targets, sems):
    copies = [pltpu.make_async_copy(s, t, sems.at[i]) for i, (s, t) in enumerate(zip(sources, targets))]
    for copy in copies:
        copy.start()
    return copies


def fetched(kernel, args, outs, flops):
    room = [pltpu.VMEM(x.shape, x.dtype) for x in args]
    args = [pltpu.with_memory_space_constraint(x, pltpu.HBM) for x in args]
    return run(
        kernel, args, outs, flops, in_specs=[HBM] * len(args),
        scratch=room + [pltpu.SemaphoreType.DMA((len(args),))],
    )


def minus_kernel(u_in, q_in, out, u, q, sems):
    for copy in fetch((u_in, q_in), (u, q), sems):
        copy.wait()
    out[...] = u[0] - penalty_rho * q[0]


def input_kernel(*refs):
    ins, out, room, sems = refs[:7], refs[7], refs[8:15], refs[15]
    p, w, b, z, order, qb, ub = room
    copies = fetch(ins, room, sems)
    copies[0].wait()
    left = split(p[0])
    copies[1].wait()
    weight = split(w[0])
    for copy in copies[2:4]:
        copy.wait()
    residual = dot3(left, weight) + b[...] - z[0]
    step = penalty_nu * dot3(split(residual), weight, NT) + penalty_rho * p[0]
    out[...] = p[0] - step_input * step
    for copy in copies[4:]:
        copy.wait()

    @pl.when(lax.axis_index("layer") == 0)
    def _():
        out[...] -= step_input * pick_rows(ub[...] - penalty_rho * qb[...], order[...])


def block_of(refs, members):
    value = refs[0][...]
    me = lax.axis_index("dp")
    for ref, those in zip(refs[1:], members[1:]):
        here = me == those[0]
        for other in those[1:]:
            here = jnp.logical_or(here, me == other)
        value = jnp.where(here, ref[...], value)
    return value


def gathered_pass(inputs, preact, outputs, duals, weight, offset, after_in, next_inputs, row_order, p_slots, z_slots, scale):
    rows, width = inputs.shape
    early_count = rows * len(p_slots)
    count = early_count + rows
    members = [[None]] + [[those for _, those in parts] for parts in p_slots]
    p_slots = [[x for x, _ in parts] for parts in p_slots]
    z_slots = [[x for x, _ in parts] for parts in z_slots]
    p_early = [[inputs]] + p_slots[:-1]
    z_early = [[preact[0]]] + z_slots[:-1]
    p_late, z_late = p_slots[-1], z_slots[-1]
    sizes = [len(parts) for parts in p_early]
    unit = 2 * rows * width * width * 3

    def group(refs, counts):
        out = []
        for n in counts:
            out.append(refs[:n])
            refs = refs[n:]
        return out

    def early_kernel(*refs):
        ins = refs[: 2 * sum(sizes)]
        w, b, z, q, u, pn, pb, order = refs[2 * sum(sizes) : 2 * sum(sizes) + 8]
        residual, kernel, z_part, q_part = refs[2 * sum(sizes) + 8 :]
        p_refs, z_refs = group(ins[: sum(sizes)], sizes), group(ins[sum(sizes) :], sizes)
        wide = split(w[0])
        blocks = [split(block_of(r, m)) for r, m in zip(p_refs, members)]
        for i, block in enumerate(blocks):
            at = slice(i * rows, (i + 1) * rows)
            residual[at] = dot3(block, wide) + b[...] - block_of(z_refs[i], members[i])
            for j in range(i + 1):
                to = slice(j * rows, (j + 1) * rows)
                piece = scale * (dot3(block, blocks[j], NT) + 1.0)
                kernel[at, to] = piece
                if j < i:
                    kernel[to, at] = piece.T
        value = z[0]
        z_part[...] = (1 - step_preact) * value - step_preact * (
            (softplus(value) - q[0]) * jax.nn.sigmoid(value)
        )
        last = lax.axis_index("layer") == lax.axis_size("layer") - 1
        after = jnp.where(last, pick_rows(pb[...], order[...]), pn[...])
        q_part[...] = u[0] + penalty_rho * after

    args = [x for parts in p_early for x in parts] + [x for parts in z_early for x in parts]
    args += [weight, offset, preact, outputs, duals, after_in, next_inputs, row_order]
    residual, kernel, z_part, q_part = run(
        early_kernel,
        args,
        [f32(early_count, width), f32(early_count, early_count), f32(rows, width), f32(rows, width)],
        unit * (2 * len(sizes)),
    )

    def solve_kernel(*refs):
        ins = refs[: sum(sizes) + len(p_late)]
        residual, kernel, w, b = refs[len(ins) : len(ins) + 4]
        w_part, b_part, pull_high, pull_low, weigh, a_part, a_pull = refs[len(ins) + 4 : len(ins) + 11]
        j_ref, turned = refs[len(ins) + 11 :]
        wide = split(w[0])
        every = [block_of(r, m) for r, m in zip(group(ins, sizes + [len(p_late)]), members)]
        late = split(every[-1])
        j_ref[:early_count, :early_count] = kernel[...]
        for i, block in enumerate(every):
            at = slice(i * rows, (i + 1) * rows)
            turned[:, at] = block.T
            piece = scale * (dot3(split(block), late, NT) + 1.0)
            j_ref[at, early_count:] = piece
            if i * rows < early_count:
                j_ref[early_count:, at] = piece.T
        j = j_ref[...]
        both = split(j)
        eye = (
            lax.broadcasted_iota(jnp.int32, (count, count), 0)
            == lax.broadcasted_iota(jnp.int32, (count, count), 1)
        ).astype(jnp.float32)
        total = eye
        for inner_step in range(1, INNER):
            total = eye + total - (dot3(both, split(total)) if inner_step > 1 else j)
        pull = scale * dot3(split(turned[...]), split(total))
        sums = scale * jnp.sum(total, axis=1, keepdims=True)
        start = jnp.concatenate([residual[...], dot3(late, wide) + b[...]], axis=0)
        new = w[0] - dot3(split(pull), split(start))
        w_part[...] = new
        new_b = b[...] - jnp.sum(sums * start, axis=0, keepdims=True)
        b_part[...] = new_b
        pull_high[...], pull_low[...] = split(pull[:, early_count:])
        weigh[...] = jnp.broadcast_to(sums[early_count:], weigh.shape)
        own = split(every[0])
        a_part[...] = dot3(own, split(new)) + new_b
        a_pull[...] = dot3(own, (pull_high[...], pull_low[...]))

    args = [x for parts in p_early + [p_late] for x in parts] + [residual, kernel, weight, offset]
    solved = run(
        solve_kernel,
        args,
        [
            f32(width, width),
            f32(1, width),
            bf16(width, rows),
            bf16(width, rows),
            f32(rows, 128),
            f32(rows, width),
            f32(rows, rows),
        ],
        unit * (3 * len(p_slots) + 4),
        scratch=[pltpu.VMEM((count, count), jnp.float32), pltpu.VMEM((width, count), jnp.float32)],
    )

    def last_kernel(*refs):
        late_refs = refs[: len(z_late)]
        w_part, b_part, pull_high, pull_low, weigh, a_part, a_pull, z_part, q_part = refs[
            len(z_late) : len(z_late) + 9
        ]
        z_out, q_out, u_out, w_out, b_out = refs[len(z_late) + 9 : len(z_late) + 14]
        z_own, q_own, u_own, w_own, b_own, sems = refs[len(z_late) + 14 :]
        value = block_of(late_refs, members[-1])
        late = split(value)
        new_w = w_part[...] + dot3((pull_high[...], pull_low[...]), late)
        w_own[0] = new_w
        copies = [pltpu.make_async_copy(w_own, w_out, sems.at[0])]
        copies[-1].start()
        shift = jnp.sum(weigh[:, :1] * value, axis=0, keepdims=True)
        b_own[...] = b_part[...] + shift
        copies.append(pltpu.make_async_copy(b_own, b_out, sems.at[1]))
        copies[-1].start()
        target = a_part[...] + shift + dot3(split(a_pull[...]), late)
        new_z = z_part[...] + step_preact * target
        z_own[0] = new_z
        copies.append(pltpu.make_async_copy(z_own, z_out, sems.at[2]))
        copies[-1].start()
        both = q_part[...]
        new_q = (penalty_nu * softplus(new_z) + both) / (penalty_nu + penalty_rho)
        q_own[0] = new_q
        copies.append(pltpu.make_async_copy(q_own, q_out, sems.at[3]))
        copies[-1].start()
        u_own[0] = both - penalty_rho * new_q
        copies.append(pltpu.make_async_copy(u_own, u_out, sems.at[4]))
        copies[-1].start()
        for copy in copies:
            copy.wait()

    one = f32(1, rows, width)
    outs = [one, one, one, f32(1, width, width), f32(1, width)]
    return run(
        last_kernel,
        list(z_late) + list(solved) + [z_part, q_part],
        outs,
        unit * 2,
        out_specs=[HBM] * len(outs),
        scratch=[pltpu.VMEM(o.shape, jnp.float32) for o in outs] + [pltpu.SemaphoreType.DMA((5,))],
    )


def gathered_body(
    layer_inputs, pre_acts, layer_outputs, multipliers, weights, biases,
    prev_outputs, prev_multipliers, next_inputs, row_order,
):
    rows, width = layer_inputs.shape[1:]
    scale = step_weight / (rows * lax.axis_size("dp"))
    unit = 2 * rows * width * width * 3
    z_slots = gather_line(pre_acts[0], "dp")
    (before,) = fetched(minus_kernel, (multipliers, layer_outputs), [f32(rows, width)], unit // 10)
    before = around(before, 1)
    (inputs,) = fetched(
        input_kernel,
        (layer_inputs, weights, biases, pre_acts, row_order, prev_outputs, prev_multipliers),
        [f32(rows, width)],
        unit * 2,
    )
    inputs = inputs - step_input * jnp.where(lax.axis_index("layer") == 0, 0.0, before)
    p_slots = gather_line(inputs, "dp")
    after_in = around(inputs, -1)
    z, q, u, w, b = gathered_pass(
        inputs, pre_acts, layer_outputs, multipliers, weights, biases,
        after_in, next_inputs, row_order, p_slots, z_slots, scale,
    )
    return (inputs[None], z, q, u, w, b)


def summed_body(
    layer_inputs,
    pre_acts,
    layer_outputs,
    multipliers,
    weights,
    biases,
    prev_outputs,
    prev_multipliers,
    next_inputs,
    row_order,
):
    row_perm = row_order[0]
    first_layer = lax.axis_index("layer") == 0
    last_layer = lax.axis_index("layer") == lax.axis_size("layer") - 1
    inputs, preact, outputs, duals = (
        layer_inputs[0],
        pre_acts[0],
        layer_outputs[0],
        multipliers[0],
    )
    weight, offset = (weights[0], biases[0])
    row_count = inputs.shape[0] * lax.axis_size("dp")
    scale = step_weight / row_count
    before = from_behind(duals - penalty_rho * outputs, "layer", 1)
    edge_before = jnp.take(prev_multipliers - penalty_rho * prev_outputs, row_perm, axis=0)
    before = jnp.where(first_layer, edge_before, before)
    residual = matmul(inputs, weight) + offset[None, :] - preact
    inputs = inputs - step_input * (
        penalty_nu * matmul(residual, weight.T) + penalty_rho * inputs + before
    )
    after_in = from_behind(inputs, "layer", -1)
    weight, offset = summed_steps(inputs, preact, weight, offset, scale)
    target = matmul(inputs, weight) + offset[None, :]
    preact = preact - step_preact * (
        preact - target + (jax.nn.softplus(preact) - outputs) * jax.nn.sigmoid(preact)
    )
    edge_inputs = jnp.take(next_inputs, row_perm, axis=0)
    after_in = jnp.where(last_layer, edge_inputs, after_in)
    outputs = (penalty_nu * jax.nn.softplus(preact) + duals + penalty_rho * after_in) / (
        penalty_nu + penalty_rho
    )
    duals = duals + penalty_rho * (after_in - outputs)
    return (inputs[None], preact[None], outputs[None], duals[None], weight[None], offset[None])


def body(*args):
    inputs = args[0]
    count = lax.axis_size("dp")
    gathers = 1 < count and inputs.shape[1] * count <= 2 * inputs.shape[2]
    return (gathered_body if gathers else summed_body)(*args)


def solution(mesh):
    return jax.shard_map(
        body,
        mesh=mesh,
        in_specs=(
            P("layer", ("groups", "dp"), None),
            P("layer", ("groups", "dp"), None),
            P("layer", ("groups", "dp"), None),
            P("layer", ("groups", "dp"), None),
            P(("groups", "layer"), None, None),
            P(("groups", "layer"), None),
            P(("groups", "dp"), None),
            P(("groups", "dp"), None),
            P(("groups", "dp"), None),
            P(("groups", "dp"), None),
        ),
        out_specs=(
            P("layer", ("groups", "dp"), None),
            P("layer", ("groups", "dp"), None),
            P("layer", ("groups", "dp"), None),
            P("layer", ("groups", "dp"), None),
            P(("groups", "layer"), None, None),
            P(("groups", "layer"), None),
        ),
        check_vma=False,
    )
```

```python
import jax
import jax.numpy as jnp
from jax import lax
from jax.experimental import pallas as pl
from jax.experimental.pallas import tpu as pltpu
from jax.sharding import PartitionSpec as P


INNER = 3


penalty_nu = 1.0
penalty_rho = 1.0
step_input = 0.2
step_weight = 0.3
step_preact = 0.5


def from_behind(x, axis, by):
    count = lax.axis_size(axis)
    pairs = [(i, i + by) for i in range(count) if 0 <= i + by < count]
    return lax.ppermute(x, axis, pairs)


def matmul(left, right):
    return jnp.dot(left, right, precision=lax.Precision.HIGHEST)


def line_plan(count):
    outbox = {(i, side): [i] for i in range(count) for side in (-1, 1)}
    rounds = []
    while any(outbox[i, side] for i in range(count) for side in (-1, 1) if 0 <= i + side < count):
        for parity in (0, 1):
            sends = []
            for i in range(count):
                side = 1 if i % 2 == parity else -1
                if 0 <= i + side < count and outbox[i, side]:
                    sends.append((i, i + side, outbox[i, side].pop(0)))
            for source, target, block in sends:
                outbox[target, target - source].append(block)
            if sends:
                rounds.append(sends)
    return rounds


def whole_swap(swaps):
    layers = lax.axis_size("layer")
    pairs = []
    for i in range(lax.axis_size("dp")):
        for l in range(layers):
            partner = l ^ 1 if layers % 2 == 0 else l
            there = (swaps[i], l) if i in swaps else (i, partner)
            pairs.append((i * layers + l, there[0] * layers + there[1]))
    return pairs


def around(x, by):
    count = lax.axis_size("layer")
    return lax.ppermute(x, "layer", [(i, (i + by) % count) for i in range(count)])


def gather_line(own, axis):
    count = lax.axis_size(axis)
    me = lax.axis_index(axis)
    held = {(i, i): own for i in range(count)}
    slots = [[] for _ in range(count - 1)]
    got = [0] * count
    for sends in line_plan(count):
        by_value = {}
        for source, target, block in sends:
            value = held[source, block]
            by_value.setdefault(id(value), (value, []))[1].append(source)
        (payload, _), *others = by_value.values()
        for value, sources in others:
            mine = jnp.any(jnp.asarray(sources) == me)
            payload = jnp.where(mine, value, payload)
        swaps = dict((s, t) for s, t, _ in sends) | dict((t, s) for s, t, _ in sends)
        arrived = lax.ppermute(payload, ("dp", "layer"), whole_swap(swaps))
        filled = {}
        for source, target, block in sends:
            held[target, block] = arrived
            filled.setdefault(got[target], []).append(target)
            got[target] += 1
        for slot, members in filled.items():
            slots[slot].append((arrived, members))
    return slots


def summed_steps(inputs, preact, weight, offset, scale):
    row_count = inputs.shape[0] * lax.axis_size("dp")
    gram_matrix, cross_term, column_sums, preact_sums = lax.psum(
        (
            matmul(inputs.T, inputs),
            matmul(inputs.T, preact),
            jnp.sum(inputs, axis=0),
            jnp.sum(preact, axis=0),
        ),
        "dp",
    )
    for _ in range(INNER):
        grad_weight = (
            matmul(gram_matrix, weight) + column_sums[:, None] * offset[None, :] - cross_term
        )
        grad_offset = matmul(column_sums[None, :], weight)[0] + row_count * offset - preact_sums
        weight = weight - scale * grad_weight
        offset = offset - scale * grad_offset
    return weight, offset


VMEM = pl.BlockSpec(memory_space=pltpu.VMEM)
HBM = pl.BlockSpec(memory_space=pltpu.HBM)
NN = (((1,), (0,)), ((), ()))
NT = (((1,), (1,)), ((), ()))


def f32(*shape):
    return jax.ShapeDtypeStruct(shape, jnp.float32)


def bf16(*shape):
    return jax.ShapeDtypeStruct(shape, jnp.bfloat16)


def run(kernel, args, outs, flops, in_specs=None, out_specs=None, scratch=(), limit=24 * 2**20):
    nbytes = sum(x.size * x.dtype.itemsize for x in (*args, *outs))
    return pl.pallas_call(
        kernel,
        out_shape=outs,
        in_specs=[VMEM] * len(args) if in_specs is None else in_specs,
        out_specs=[VMEM] * len(outs) if out_specs is None else out_specs,
        scratch_shapes=scratch,
        cost_estimate=pl.CostEstimate(flops=flops, bytes_accessed=nbytes, transcendentals=0),
        compiler_params=pltpu.CompilerParams(vmem_limit_bytes=limit),
    )(*args)


def split(x):
    high = x.astype(jnp.bfloat16)
    return high, (x - high.astype(jnp.float32)).astype(jnp.bfloat16)


def dot3(left, right, dims=NN):
    one = lambda a, b: lax.dot_general(a, b, dims, preferred_element_type=jnp.float32)
    return one(left[0], right[0]) + (one(left[0], right[1]) + one(left[1], right[0]))


def pick_rows(rows, order):
    count = rows.shape[0]
    hot = (lax.broadcasted_iota(jnp.int32, (count, count), 0) == order).astype(jnp.float32)
    hot = hot.T.astype(jnp.bfloat16)
    high, low = split(rows)
    rest = (rows - high.astype(jnp.float32) - low.astype(jnp.float32)).astype(jnp.bfloat16)
    one = lambda b: lax.dot_general(hot, b, NN, preferred_element_type=jnp.float32)
    return one(high) + (one(low) + one(rest))


def softplus(v):
    return jnp.maximum(v, 0.0) + jnp.log(1.0 + jnp.exp(-jnp.abs(v)))


def fetch(sources, targets, sems):
    copies = [pltpu.make_async_copy(s, t, sems.at[i]) for i, (s, t) in enumerate(zip(sources, targets))]
    for copy in copies:
        copy.start()
    return copies


def first_kernel(u_in, q_in, *refs):
    count = (len(refs) - 4) // 2
    sources, out, targets = refs[:count], refs[count], refs[count + 1 : 2 * count + 1]
    u, q, sems = refs[2 * count + 1 :]
    copies = fetch((u_in, q_in) + sources, (u, q) + targets, sems)
    for copy in copies[:2]:
        copy.wait()
    out[...] = u[0] - penalty_rho * q[0]
    for copy in copies[2:]:
        copy.wait()


def input_kernel(p, w, b, z, order, qb, ub, out):
    weight = split(w[0])
    residual = dot3(split(p[0]), weight) + b[...] - z[0]
    step = penalty_nu * dot3(split(residual), weight, NT) + penalty_rho * p[0]
    out[...] = p[0] - step_input * step

    @pl.when(lax.axis_index("layer") == 0)
    def _():
        out[...] -= step_input * pick_rows(ub[...] - penalty_rho * qb[...], order[...])


def block_of(refs, members):
    value = refs[0][...]
    me = lax.axis_index("dp")
    for ref, those in zip(refs[1:], members[1:]):
        here = me == those[0]
        for other in those[1:]:
            here = jnp.logical_or(here, me == other)
        value = jnp.where(here, ref[...], value)
    return value


def gathered_pass(inputs, preact, outputs, duals, weight, offset, after_in, next_inputs, row_order, p_slots, z_slots, scale):
    rows, width = inputs.shape
    early_count = rows * len(p_slots)
    count = early_count + rows
    members = [[None]] + [[those for _, those in parts] for parts in p_slots]
    p_slots = [[x for x, _ in parts] for parts in p_slots]
    z_slots = [[x for x, _ in parts] for parts in z_slots]
    p_early = [[inputs]] + p_slots[:-1]
    z_early = [[preact[0]]] + z_slots[:-1]
    p_late, z_late = p_slots[-1], z_slots[-1]
    sizes = [len(parts) for parts in p_early]
    unit = 2 * rows * width * width * 3

    def group(refs, counts):
        out = []
        for n in counts:
            out.append(refs[:n])
            refs = refs[n:]
        return out

    def early_kernel(*refs):
        ins = refs[: 2 * sum(sizes)]
        w, b, z, q, u, pn, pb, order = refs[2 * sum(sizes) : 2 * sum(sizes) + 8]
        residual, kernel, z_part, q_part = refs[2 * sum(sizes) + 8 :]
        p_refs, z_refs = group(ins[: sum(sizes)], sizes), group(ins[sum(sizes) :], sizes)
        wide = split(w[0])
        blocks = [split(block_of(r, m)) for r, m in zip(p_refs, members)]
        for i, block in enumerate(blocks):
            at = slice(i * rows, (i + 1) * rows)
            residual[at] = dot3(block, wide) + b[...] - block_of(z_refs[i], members[i])
            for j in range(i + 1):
                to = slice(j * rows, (j + 1) * rows)
                piece = scale * (dot3(block, blocks[j], NT) + 1.0)
                kernel[at, to] = piece
                if j < i:
                    kernel[to, at] = piece.T
        value = z[0]
        z_part[...] = (1 - step_preact) * value - step_preact * (
            (softplus(value) - q[0]) * jax.nn.sigmoid(value)
        )
        last = lax.axis_index("layer") == lax.axis_size("layer") - 1
        after = jnp.where(last, pick_rows(pb[...], order[...]), pn[...])
        q_part[...] = u[0] + penalty_rho * after

    args = [x for parts in p_early for x in parts] + [x for parts in z_early for x in parts]
    args += [weight, offset, preact, outputs, duals, after_in, next_inputs, row_order]
    residual, kernel, z_part, q_part = run(
        early_kernel,
        args,
        [f32(early_count, width), f32(early_count, early_count), f32(rows, width), f32(rows, width)],
        unit * (2 * len(sizes)),
    )

    def solve_kernel(*refs):
        ins = refs[: sum(sizes) + len(p_late)]
        residual, kernel, w, b = refs[len(ins) : len(ins) + 4]
        w_part, b_part, pull_high, pull_low, weigh, a_part, a_pull = refs[len(ins) + 4 : len(ins) + 11]
        j_ref, turned = refs[len(ins) + 11 :]
        wide = split(w[0])
        every = [block_of(r, m) for r, m in zip(group(ins, sizes + [len(p_late)]), members)]
        late = split(every[-1])
        j_ref[:early_count, :early_count] = kernel[...]
        for i, block in enumerate(every):
            at = slice(i * rows, (i + 1) * rows)
            turned[:, at] = block.T
            piece = scale * (dot3(split(block), late, NT) + 1.0)
            j_ref[at, early_count:] = piece
            if i * rows < early_count:
                j_ref[early_count:, at] = piece.T
        j = j_ref[...]
        both = split(j)
        eye = (
            lax.broadcasted_iota(jnp.int32, (count, count), 0)
            == lax.broadcasted_iota(jnp.int32, (count, count), 1)
        ).astype(jnp.float32)
        total = eye
        for inner_step in range(1, INNER):
            total = eye + total - (dot3(both, split(total)) if inner_step > 1 else j)
        pull = scale * dot3(split(turned[...]), split(total))
        sums = scale * jnp.sum(total, axis=1, keepdims=True)
        start = jnp.concatenate([residual[...], dot3(late, wide) + b[...]], axis=0)
        new = w[0] - dot3(split(pull), split(start))
        w_part[...] = new
        new_b = b[...] - jnp.sum(sums * start, axis=0, keepdims=True)
        b_part[...] = new_b
        pull_high[...], pull_low[...] = split(pull[:, early_count:])
        weigh[...] = jnp.broadcast_to(sums[early_count:], weigh.shape)
        own = split(every[0])
        a_part[...] = dot3(own, split(new)) + new_b
        a_pull[...] = dot3(own, (pull_high[...], pull_low[...]))

    args = [x for parts in p_early + [p_late] for x in parts] + [residual, kernel, weight, offset]
    solved = run(
        solve_kernel,
        args,
        [
            f32(width, width),
            f32(1, width),
            bf16(width, rows),
            bf16(width, rows),
            f32(rows, 128),
            f32(rows, width),
            f32(rows, rows),
        ],
        unit * (3 * len(p_slots) + 4),
        scratch=[pltpu.VMEM((count, count), jnp.float32), pltpu.VMEM((width, count), jnp.float32)],
    )

    w_chunks = [slice(i * width // 4, (i + 1) * width // 4) for i in range(4)]
    z_chunks = [slice(i * rows // 2, (i + 1) * rows // 2) for i in range(2)]

    def last_kernel(*refs):
        late_refs = refs[: len(z_late)]
        w_part, b_part, pull_high, pull_low, weigh, a_part, a_pull, z_part, q_part = refs[
            len(z_late) : len(z_late) + 9
        ]
        z_out, q_out, u_out, w_out, b_out = refs[len(z_late) + 9 : len(z_late) + 14]
        z_own, q_own, u_own, w_own, b_own, sems = refs[len(z_late) + 14 :]
        value = block_of(late_refs, members[-1])
        late = split(value)
        copies = []

        def send(own, out, at):
            copies.append(pltpu.make_async_copy(own.at[0, at], out.at[0, at], sems.at[len(copies)]))
            copies[-1].start()

        for at in w_chunks:
            w_own[0, at] = w_part[at] + dot3((pull_high[at], pull_low[at]), late)
            send(w_own, w_out, at)
        shift = jnp.sum(weigh[:, :1] * value, axis=0, keepdims=True)
        b_own[...] = b_part[...] + shift
        copies.append(pltpu.make_async_copy(b_own, b_out, sems.at[len(copies)]))
        copies[-1].start()
        for at in z_chunks:
            target = a_part[at] + shift + dot3(split(a_pull[at]), late)
            new_z = z_part[at] + step_preact * target
            z_own[0, at] = new_z
            send(z_own, z_out, at)
            both = q_part[at]
            new_q = (penalty_nu * softplus(new_z) + both) / (penalty_nu + penalty_rho)
            q_own[0, at] = new_q
            send(q_own, q_out, at)
            u_own[0, at] = both - penalty_rho * new_q
            send(u_own, u_out, at)
        for copy in copies:
            copy.wait()

    one = f32(1, rows, width)
    outs = [one, one, one, f32(1, width, width), f32(1, width)]
    return run(
        last_kernel,
        list(z_late) + list(solved) + [z_part, q_part],
        outs,
        unit * 2,
        out_specs=[HBM] * len(outs),
        scratch=[pltpu.VMEM(o.shape, jnp.float32) for o in outs] + [pltpu.SemaphoreType.DMA((len(w_chunks) + 3 * len(z_chunks) + 1,))],
    )


def gathered_body(
    layer_inputs, pre_acts, layer_outputs, multipliers, weights, biases,
    prev_outputs, prev_multipliers, next_inputs, row_order,
):
    rows, width = layer_inputs.shape[1:]
    scale = step_weight / (rows * lax.axis_size("dp"))
    unit = 2 * rows * width * width * 3
    z_slots = gather_line(pre_acts[0], "dp")
    shared = (layer_inputs, weights, biases, pre_acts)
    hbm = [
        pltpu.with_memory_space_constraint(x, pltpu.HBM)
        for x in (multipliers, layer_outputs) + shared
    ]
    one = pltpu.VMEM((1, rows, width), jnp.float32)
    before, p_near, w_near, b_near, z_near = run(
        first_kernel,
        hbm,
        [f32(rows, width)] + [f32(*x.shape) for x in shared],
        unit // 10,
        in_specs=[HBM] * len(hbm),
        scratch=[one, one, pltpu.SemaphoreType.DMA((len(hbm),))],
    )
    before = around(before, 1)
    (inputs,) = run(
        input_kernel,
        (p_near, w_near, b_near, z_near, row_order, prev_outputs, prev_multipliers),
        [f32(rows, width)],
        unit * 2,
    )
    inputs = inputs - step_input * jnp.where(lax.axis_index("layer") == 0, 0.0, before)
    p_slots = gather_line(inputs, "dp")
    after_in = around(inputs, -1)
    z, q, u, w, b = gathered_pass(
        inputs, z_near, layer_outputs, multipliers, w_near, b_near,
        after_in, next_inputs, row_order, p_slots, z_slots, scale,
    )
    return (inputs[None], z, q, u, w, b)


def summed_body(
    layer_inputs,
    pre_acts,
    layer_outputs,
    multipliers,
    weights,
    biases,
    prev_outputs,
    prev_multipliers,
    next_inputs,
    row_order,
):
    row_perm = row_order[0]
    first_layer = lax.axis_index("layer") == 0
    last_layer = lax.axis_index("layer") == lax.axis_size("layer") - 1
    inputs, preact, outputs, duals = (
        layer_inputs[0],
        pre_acts[0],
        layer_outputs[0],
        multipliers[0],
    )
    weight, offset = (weights[0], biases[0])
    row_count = inputs.shape[0] * lax.axis_size("dp")
    scale = step_weight / row_count
    before = from_behind(duals - penalty_rho * outputs, "layer", 1)
    edge_before = jnp.take(prev_multipliers - penalty_rho * prev_outputs, row_perm, axis=0)
    before = jnp.where(first_layer, edge_before, before)
    residual = matmul(inputs, weight) + offset[None, :] - preact
    inputs = inputs - step_input * (
        penalty_nu * matmul(residual, weight.T) + penalty_rho * inputs + before
    )
    after_in = from_behind(inputs, "layer", -1)
    weight, offset = summed_steps(inputs, preact, weight, offset, scale)
    target = matmul(inputs, weight) + offset[None, :]
    preact = preact - step_preact * (
        preact - target + (jax.nn.softplus(preact) - outputs) * jax.nn.sigmoid(preact)
    )
    edge_inputs = jnp.take(next_inputs, row_perm, axis=0)
    after_in = jnp.where(last_layer, edge_inputs, after_in)
    outputs = (penalty_nu * jax.nn.softplus(preact) + duals + penalty_rho * after_in) / (
        penalty_nu + penalty_rho
    )
    duals = duals + penalty_rho * (after_in - outputs)
    return (inputs[None], preact[None], outputs[None], duals[None], weight[None], offset[None])


def body(*args):
    inputs = args[0]
    count = lax.axis_size("dp")
    gathers = 1 < count and inputs.shape[1] * count <= 2 * inputs.shape[2]
    return (gathered_body if gathers else summed_body)(*args)


def solution(mesh):
    return jax.shard_map(
        body,
        mesh=mesh,
        in_specs=(
            P("layer", ("groups", "dp"), None),
            P("layer", ("groups", "dp"), None),
            P("layer", ("groups", "dp"), None),
            P("layer", ("groups", "dp"), None),
            P(("groups", "layer"), None, None),
            P(("groups", "layer"), None),
            P(("groups", "dp"), None),
            P(("groups", "dp"), None),
            P(("groups", "dp"), None),
            P(("groups", "dp"), None),
        ),
        out_specs=(
            P("layer", ("groups", "dp"), None),
            P("layer", ("groups", "dp"), None),
            P("layer", ("groups", "dp"), None),
            P("layer", ("groups", "dp"), None),
            P(("groups", "layer"), None, None),
            P(("groups", "layer"), None),
        ),
        check_vma=False,
    )
```

```python
import jax
import jax.numpy as jnp
from jax import lax
from jax.experimental import pallas as pl
from jax.experimental.pallas import tpu as pltpu
from jax.sharding import PartitionSpec as P


INNER = 3


penalty_nu = 1.0
penalty_rho = 1.0
step_input = 0.2
step_weight = 0.3
step_preact = 0.5


def from_behind(x, axis, by):
    count = lax.axis_size(axis)
    pairs = [(i, i + by) for i in range(count) if 0 <= i + by < count]
    return lax.ppermute(x, axis, pairs)


def matmul(left, right):
    return jnp.dot(left, right, precision=lax.Precision.HIGHEST)


def line_plan(count):
    outbox = {(i, side): [i] for i in range(count) for side in (-1, 1)}
    rounds = []
    while any(outbox[i, side] for i in range(count) for side in (-1, 1) if 0 <= i + side < count):
        for parity in (0, 1):
            sends = []
            for i in range(count):
                side = 1 if i % 2 == parity else -1
                if 0 <= i + side < count and outbox[i, side]:
                    sends.append((i, i + side, outbox[i, side].pop(0)))
            for source, target, block in sends:
                outbox[target, target - source].append(block)
            if sends:
                rounds.append(sends)
    return rounds


def whole_swap(swaps):
    layers = lax.axis_size("layer")
    pairs = []
    for i in range(lax.axis_size("dp")):
        for l in range(layers):
            partner = l ^ 1 if layers % 2 == 0 else l
            there = (swaps[i], l) if i in swaps else (i, partner)
            pairs.append((i * layers + l, there[0] * layers + there[1]))
    return pairs


def around(x, by):
    count = lax.axis_size("layer")
    return lax.ppermute(x, "layer", [(i, (i + by) % count) for i in range(count)])


def gather_line(own, axis):
    count = lax.axis_size(axis)
    me = lax.axis_index(axis)
    held = {(i, i): own for i in range(count)}
    slots = [[] for _ in range(count - 1)]
    got = [0] * count
    for sends in line_plan(count):
        by_value = {}
        for source, target, block in sends:
            value = held[source, block]
            by_value.setdefault(id(value), (value, []))[1].append(source)
        (payload, _), *others = by_value.values()
        for value, sources in others:
            mine = jnp.any(jnp.asarray(sources) == me)
            payload = jnp.where(mine, value, payload)
        swaps = dict((s, t) for s, t, _ in sends) | dict((t, s) for s, t, _ in sends)
        arrived = lax.ppermute(payload, ("dp", "layer"), whole_swap(swaps))
        filled = {}
        for source, target, block in sends:
            held[target, block] = arrived
            filled.setdefault(got[target], []).append(target)
            got[target] += 1
        for slot, members in filled.items():
            slots[slot].append((arrived, members))
    return slots


def summed_steps(inputs, preact, weight, offset, scale):
    row_count = inputs.shape[0] * lax.axis_size("dp")
    gram_matrix, cross_term, column_sums, preact_sums = lax.psum(
        (
            matmul(inputs.T, inputs),
            matmul(inputs.T, preact),
            jnp.sum(inputs, axis=0),
            jnp.sum(preact, axis=0),
        ),
        "dp",
    )
    for _ in range(INNER):
        grad_weight = (
            matmul(gram_matrix, weight) + column_sums[:, None] * offset[None, :] - cross_term
        )
        grad_offset = matmul(column_sums[None, :], weight)[0] + row_count * offset - preact_sums
        weight = weight - scale * grad_weight
        offset = offset - scale * grad_offset
    return weight, offset


VMEM = pl.BlockSpec(memory_space=pltpu.VMEM)
HBM = pl.BlockSpec(memory_space=pltpu.HBM)
NN = (((1,), (0,)), ((), ()))
NT = (((1,), (1,)), ((), ()))


def f32(*shape):
    return jax.ShapeDtypeStruct(shape, jnp.float32)


def bf16(*shape):
    return jax.ShapeDtypeStruct(shape, jnp.bfloat16)


def run(kernel, args, outs, flops, in_specs=None, out_specs=None, scratch=(), limit=24 * 2**20):
    nbytes = sum(x.size * x.dtype.itemsize for x in (*args, *outs))
    return pl.pallas_call(
        kernel,
        out_shape=outs,
        in_specs=[VMEM] * len(args) if in_specs is None else in_specs,
        out_specs=[VMEM] * len(outs) if out_specs is None else out_specs,
        scratch_shapes=scratch,
        cost_estimate=pl.CostEstimate(flops=flops, bytes_accessed=nbytes, transcendentals=0),
        compiler_params=pltpu.CompilerParams(vmem_limit_bytes=limit),
    )(*args)


def split(x):
    high = x.astype(jnp.bfloat16)
    return high, (x - high.astype(jnp.float32)).astype(jnp.bfloat16)


def dot3(left, right, dims=NN):
    one = lambda a, b: lax.dot_general(a, b, dims, preferred_element_type=jnp.float32)
    return one(left[0], right[0]) + (one(left[0], right[1]) + one(left[1], right[0]))


def pick_rows(rows, order):
    count = rows.shape[0]
    hot = (lax.broadcasted_iota(jnp.int32, (count, count), 0) == order).astype(jnp.float32)
    hot = hot.T.astype(jnp.bfloat16)
    high, low = split(rows)
    rest = (rows - high.astype(jnp.float32) - low.astype(jnp.float32)).astype(jnp.bfloat16)
    one = lambda b: lax.dot_general(hot, b, NN, preferred_element_type=jnp.float32)
    return one(high) + (one(low) + one(rest))


def softplus(v):
    return jnp.maximum(v, 0.0) + jnp.log(1.0 + jnp.exp(-jnp.abs(v)))


def fetch(sources, targets, sems):
    copies = [pltpu.make_async_copy(s, t, sems.at[i]) for i, (s, t) in enumerate(zip(sources, targets))]
    for copy in copies:
        copy.start()
    return copies


def first_kernel(u_in, q_in, *refs):
    count = (len(refs) - 4) // 2
    sources, out, targets = refs[:count], refs[count], refs[count + 1 : 2 * count + 1]
    u, q, sems = refs[2 * count + 1 :]
    copies = fetch((u_in, q_in) + sources, (u, q) + targets, sems)
    for copy in copies[:2]:
        copy.wait()
    out[...] = u[0] - penalty_rho * q[0]
    for copy in copies[2:]:
        copy.wait()


def input_kernel(p, w, b, z, order, qb, ub, out):
    weight = split(w[0])
    residual = dot3(split(p[0]), weight) + b[...] - z[0]
    step = penalty_nu * dot3(split(residual), weight, NT) + penalty_rho * p[0]
    out[...] = p[0] - step_input * step

    @pl.when(lax.axis_index("layer") == 0)
    def _():
        out[...] -= step_input * pick_rows(ub[...] - penalty_rho * qb[...], order[...])


def block_of(refs, members):
    value = refs[0][...]
    me = lax.axis_index("dp")
    for ref, those in zip(refs[1:], members[1:]):
        here = me == those[0]
        for other in those[1:]:
            here = jnp.logical_or(here, me == other)
        value = jnp.where(here, ref[...], value)
    return value


def gathered_pass(inputs, preact, outputs, duals, weight, offset, after_in, next_inputs, row_order, p_slots, z_slots, scale):
    rows, width = inputs.shape
    early_count = rows * len(p_slots)
    count = early_count + rows
    members = [[None]] + [[those for _, those in parts] for parts in p_slots]
    p_slots = [[x for x, _ in parts] for parts in p_slots]
    z_slots = [[x for x, _ in parts] for parts in z_slots]
    p_early = [[inputs]] + p_slots[:-1]
    z_early = [[preact[0]]] + z_slots[:-1]
    p_late, z_late = p_slots[-1], z_slots[-1]
    sizes = [len(parts) for parts in p_early]
    unit = 2 * rows * width * width * 3

    def group(refs, counts):
        out = []
        for n in counts:
            out.append(refs[:n])
            refs = refs[n:]
        return out

    def early_kernel(*refs):
        ins = refs[: 2 * sum(sizes)]
        w, b, z, q, u, pn, pb, order = refs[2 * sum(sizes) : 2 * sum(sizes) + 8]
        residual, kernel, square, turned, z_part, q_part = refs[2 * sum(sizes) + 8 :]
        p_refs, z_refs = group(ins[: sum(sizes)], sizes), group(ins[sum(sizes) :], sizes)
        wide = split(w[0])
        whole = [block_of(r, m) for r, m in zip(p_refs, members)]
        blocks = [split(block) for block in whole]
        for i, block in enumerate(blocks):
            at = slice(i * rows, (i + 1) * rows)
            turned[:, at] = whole[i].T
            residual[at] = dot3(block, wide) + b[...] - block_of(z_refs[i], members[i])
            for j in range(i + 1):
                to = slice(j * rows, (j + 1) * rows)
                piece = scale * (dot3(block, blocks[j], NT) + 1.0)
                kernel[at, to] = piece
                if j < i:
                    kernel[to, at] = piece.T
        both = split(kernel[...])
        square[...] = dot3(both, both)
        value = z[0]
        z_part[...] = (1 - step_preact) * value - step_preact * (
            (softplus(value) - q[0]) * jax.nn.sigmoid(value)
        )
        last = lax.axis_index("layer") == lax.axis_size("layer") - 1
        after = jnp.where(last, pick_rows(pb[...], order[...]), pn[...])
        q_part[...] = u[0] + penalty_rho * after

    args = [x for parts in p_early for x in parts] + [x for parts in z_early for x in parts]
    args += [weight, offset, preact, outputs, duals, after_in, next_inputs, row_order]
    residual, kernel, square, turned, z_part, q_part = run(
        early_kernel,
        args,
        [
            f32(early_count, width),
            f32(early_count, early_count),
            f32(early_count, early_count),
            f32(width, early_count),
            f32(rows, width),
            f32(rows, width),
        ],
        unit * (3 * len(sizes)),
    )

    def solve_kernel(*refs):
        ins = refs[: sum(sizes) + len(p_late)]
        residual, kernel, square, turned, w, b = refs[len(ins) : len(ins) + 6]
        w_part, b_part, pull_high, pull_low, weigh, a_part, a_pull = refs[len(ins) + 6 : len(ins) + 13]
        total_ref, turned_ref = refs[len(ins) + 13 :]
        wide = split(w[0])
        every = [block_of(r, m) for r, m in zip(group(ins, sizes + [len(p_late)]), members)]
        late = split(every[-1])
        turned_ref[:, :early_count] = turned[...]
        turned_ref[:, early_count:] = every[-1].T
        edge = jnp.concatenate([scale * (dot3(split(x), late, NT) + 1.0) for x in every[:-1]], axis=0)
        corner = scale * (dot3(late, late, NT) + 1.0)
        edge_across, near = edge.T, kernel[...]
        edge_split, across_split, corner_split = split(edge), split(edge_across), split(corner)
        mixed = dot3(split(near), edge_split) + dot3(edge_split, corner_split) - INNER * edge
        total_ref[:early_count, :early_count] = square[...] + dot3(edge_split, across_split) - INNER * near
        total_ref[:early_count, early_count:] = mixed
        total_ref[early_count:, :early_count] = mixed.T
        total_ref[early_count:, early_count:] = (
            dot3(across_split, edge_split) + dot3(corner_split, corner_split) - INNER * corner
        )
        eye = (
            lax.broadcasted_iota(jnp.int32, (count, count), 0)
            == lax.broadcasted_iota(jnp.int32, (count, count), 1)
        ).astype(jnp.float32)
        total = total_ref[...] + INNER * eye
        pull = scale * dot3(split(turned_ref[...]), split(total))
        sums = scale * jnp.sum(total, axis=1, keepdims=True)
        start = jnp.concatenate([residual[...], dot3(late, wide) + b[...]], axis=0)
        new = w[0] - dot3(split(pull), split(start))
        w_part[...] = new
        new_b = b[...] - jnp.sum(sums * start, axis=0, keepdims=True)
        b_part[...] = new_b
        pull_high[...], pull_low[...] = split(pull[:, early_count:])
        weigh[...] = jnp.broadcast_to(sums[early_count:], weigh.shape)
        own = split(every[0])
        a_part[...] = dot3(own, split(new)) + new_b
        a_pull[...] = dot3(own, (pull_high[...], pull_low[...]))

    args = [x for parts in p_early + [p_late] for x in parts] + [residual, kernel, square, turned, weight, offset]
    solved = run(
        solve_kernel,
        args,
        [
            f32(width, width),
            f32(1, width),
            bf16(width, rows),
            bf16(width, rows),
            f32(rows, 128),
            f32(rows, width),
            f32(rows, rows),
        ],
        unit * (3 * len(p_slots) + 4),
        scratch=[pltpu.VMEM((count, count), jnp.float32), pltpu.VMEM((width, count), jnp.float32)],
    )

    w_chunks = [slice(i * width // 4, (i + 1) * width // 4) for i in range(4)]
    z_chunks = [slice(i * rows // 2, (i + 1) * rows // 2) for i in range(2)]

    def last_kernel(*refs):
        late_refs = refs[: len(z_late)]
        w_part, b_part, pull_high, pull_low, weigh, a_part, a_pull, z_part, q_part = refs[
            len(z_late) : len(z_late) + 9
        ]
        z_out, q_out, u_out, w_out, b_out = refs[len(z_late) + 9 : len(z_late) + 14]
        z_own, q_own, u_own, w_own, b_own, sems = refs[len(z_late) + 14 :]
        value = block_of(late_refs, members[-1])
        late = split(value)
        copies = []

        def send(own, out, at):
            copies.append(pltpu.make_async_copy(own.at[0, at], out.at[0, at], sems.at[len(copies)]))
            copies[-1].start()

        shift = jnp.sum(weigh[:, :1] * value, axis=0, keepdims=True)
        b_own[...] = b_part[...] + shift
        copies.append(pltpu.make_async_copy(b_own, b_out, sems.at[len(copies)]))
        copies[-1].start()
        for at in z_chunks:
            target = a_part[at] + shift + dot3(split(a_pull[at]), late)
            new_z = z_part[at] + step_preact * target
            z_own[0, at] = new_z
            send(z_own, z_out, at)
            both = q_part[at]
            new_q = (penalty_nu * softplus(new_z) + both) / (penalty_nu + penalty_rho)
            q_own[0, at] = new_q
            send(q_own, q_out, at)
            u_own[0, at] = both - penalty_rho * new_q
            send(u_own, u_out, at)
        for at in w_chunks:
            w_own[0, at] = w_part[at] + dot3((pull_high[at], pull_low[at]), late)
            send(w_own, w_out, at)
        for copy in copies:
            copy.wait()

    one = f32(1, rows, width)
    outs = [one, one, one, f32(1, width, width), f32(1, width)]
    return run(
        last_kernel,
        list(z_late) + list(solved) + [z_part, q_part],
        outs,
        unit * 2,
        out_specs=[HBM] * len(outs),
        scratch=[pltpu.VMEM(o.shape, jnp.float32) for o in outs] + [pltpu.SemaphoreType.DMA((len(w_chunks) + 3 * len(z_chunks) + 1,))],
    )


def gathered_body(
    layer_inputs, pre_acts, layer_outputs, multipliers, weights, biases,
    prev_outputs, prev_multipliers, next_inputs, row_order,
):
    rows, width = layer_inputs.shape[1:]
    scale = step_weight / (rows * lax.axis_size("dp"))
    unit = 2 * rows * width * width * 3
    z_slots = gather_line(pre_acts[0], "dp")
    shared = (layer_inputs, weights, biases, pre_acts)
    hbm = [
        pltpu.with_memory_space_constraint(x, pltpu.HBM)
        for x in (multipliers, layer_outputs) + shared
    ]
    one = pltpu.VMEM((1, rows, width), jnp.float32)
    before, p_near, w_near, b_near, z_near = run(
        first_kernel,
        hbm,
        [f32(rows, width)] + [f32(*x.shape) for x in shared],
        unit // 10,
        in_specs=[HBM] * len(hbm),
        scratch=[one, one, pltpu.SemaphoreType.DMA((len(hbm),))],
    )
    before = around(before, 1)
    (inputs,) = run(
        input_kernel,
        (p_near, w_near, b_near, z_near, row_order, prev_outputs, prev_multipliers),
        [f32(rows, width)],
        unit * 2,
    )
    inputs = inputs - step_input * jnp.where(lax.axis_index("layer") == 0, 0.0, before)
    p_slots = gather_line(inputs, "dp")
    after_in = around(inputs, -1)
    z, q, u, w, b = gathered_pass(
        inputs, z_near, layer_outputs, multipliers, w_near, b_near,
        after_in, next_inputs, row_order, p_slots, z_slots, scale,
    )
    return (inputs[None], z, q, u, w, b)


def summed_body(
    layer_inputs,
    pre_acts,
    layer_outputs,
    multipliers,
    weights,
    biases,
    prev_outputs,
    prev_multipliers,
    next_inputs,
    row_order,
):
    row_perm = row_order[0]
    first_layer = lax.axis_index("layer") == 0
    last_layer = lax.axis_index("layer") == lax.axis_size("layer") - 1
    inputs, preact, outputs, duals = (
        layer_inputs[0],
        pre_acts[0],
        layer_outputs[0],
        multipliers[0],
    )
    weight, offset = (weights[0], biases[0])
    row_count = inputs.shape[0] * lax.axis_size("dp")
    scale = step_weight / row_count
    before = from_behind(duals - penalty_rho * outputs, "layer", 1)
    edge_before = jnp.take(prev_multipliers - penalty_rho * prev_outputs, row_perm, axis=0)
    before = jnp.where(first_layer, edge_before, before)
    residual = matmul(inputs, weight) + offset[None, :] - preact
    inputs = inputs - step_input * (
        penalty_nu * matmul(residual, weight.T) + penalty_rho * inputs + before
    )
    after_in = from_behind(inputs, "layer", -1)
    weight, offset = summed_steps(inputs, preact, weight, offset, scale)
    target = matmul(inputs, weight) + offset[None, :]
    preact = preact - step_preact * (
        preact - target + (jax.nn.softplus(preact) - outputs) * jax.nn.sigmoid(preact)
    )
    edge_inputs = jnp.take(next_inputs, row_perm, axis=0)
    after_in = jnp.where(last_layer, edge_inputs, after_in)
    outputs = (penalty_nu * jax.nn.softplus(preact) + duals + penalty_rho * after_in) / (
        penalty_nu + penalty_rho
    )
    duals = duals + penalty_rho * (after_in - outputs)
    return (inputs[None], preact[None], outputs[None], duals[None], weight[None], offset[None])


def body(*args):
    inputs = args[0]
    count = lax.axis_size("dp")
    gathers = INNER == 3 and 1 < count and inputs.shape[1] * count <= 2 * inputs.shape[2]
    return (gathered_body if gathers else summed_body)(*args)


def solution(mesh):
    return jax.shard_map(
        body,
        mesh=mesh,
        in_specs=(
            P("layer", ("groups", "dp"), None),
            P("layer", ("groups", "dp"), None),
            P("layer", ("groups", "dp"), None),
            P("layer", ("groups", "dp"), None),
            P(("groups", "layer"), None, None),
            P(("groups", "layer"), None),
            P(("groups", "dp"), None),
            P(("groups", "dp"), None),
            P(("groups", "dp"), None),
            P(("groups", "dp"), None),
        ),
        out_specs=(
            P("layer", ("groups", "dp"), None),
            P("layer", ("groups", "dp"), None),
            P("layer", ("groups", "dp"), None),
            P("layer", ("groups", "dp"), None),
            P(("groups", "layer"), None, None),
            P(("groups", "layer"), None),
        ),
        check_vma=False,
    )
```
